256 devices in a mesh: grp: 4 (over y, x), seq: 32 (over z), tp: 2 (over core).
Axes of the slice: x: 2, y: 2, z: 32, core: 2. Of those that a mesh axis runs over, the one named last changes fastest.
The devices are a block of a 4x8x32 slice.
Arguments:
- visual_q: bfloat16 [32768, 1536], P(('grp', 'seq'), 'tp'), parts along dimension 0, may hold values from -8 to 8
- visual_key_input: bfloat16 [32768, 1536], P(('grp', 'seq'), 'tp'), parts along dimension 0, may hold values from -8 to 8
- visual_v: bfloat16 [32768, 1536], P(('grp', 'seq'), 'tp'), parts along dimension 0, may hold values from -6 to 6
- text_k: bfloat16 [1024, 1536], P(('grp', 'seq'), 'tp'), parts along dimension 0, may hold values from -6 to 6
- text_v: bfloat16 [1024, 1536], P(('grp', 'seq'), 'tp'), parts along dimension 0, may hold values from -6 to 6
- text_mask: int32 [1024], P(('grp', 'seq')), parts along dimension 0, may hold values from 0 to 1, as said below
- slab_order: int32 [128], P(('grp', 'seq')), parts along dimension 0, may hold values from 0 to 31, each once
- q_gain: float32 [128], replicated, may hold values from 0.8 to 6
- key_norm_gain: float32 [128], replicated, may hold values from 0.8 to 6
- w_out: bfloat16 [1536, 3072], P('tp'), may hold values from -0.8984375 to 0.8984375
Outputs:
- attended: bfloat16 [32768, 3072], P(('grp', 'seq', 'tp')), parts along dimension 0
The draws below stay inside these ranges and needn't reach their ends.
There are 4 independent parts, one for each index of `grp`. The reference program is written for one: setup_inputs(seed, part) draws one part's arguments, and reference() takes and returns one part's arrays. A program takes and returns all parts, laid end to end along the dimension named above; an argument that names none is the same for every part. Nothing has to cross between parts.
Inputs may be any that keep to these rules, and one draw needn't show every extreme that they name: `text_mask`: the first entries are 1 and the rest 0, with at least 32 ones. `slab_order`: each slab number once.
All inputs are finite; a program needn't handle non-finite values.
Results may differ from the reference program's by a relative error of at most 0.013.
The reference program's roundings to bfloat16 on the way count: a program that leaves them out, or rounds other values in their place, can miss the bound.
Values may be sent and summed in bfloat16 or wider, within the bound.
No kernel may reach another device: no remote copies, remote signals or barrier semaphores. Data moves between devices by JAX's collectives and lax.ppermute only.
A program may use at most 128 MiB of HBM per device.

```python
import jax
import jax.numpy as jnp
from jax import lax

HEADS = 12
HEAD = 128
D = 3072
TEXT = 256
SLAB_H = 2
WIDE = 32
TOK_DEV = 256
VIS = 8192
N_SEQ = 32
N_TP = 2


def shared_rows(key):
    return jnp.clip(jax.random.normal(jax.random.fold_in(key, 101), (VIS, HEADS * HEAD), jnp.float32), -8.0, 8.0)


def draw_visual_key_input(key, part):
    return shared_rows(key).astype(jnp.bfloat16)


def draw_visual_q(key, part):
    fresh = jnp.clip(jax.random.normal(jax.random.fold_in(key, 202), (VIS, HEADS * HEAD), jnp.float32), -8.0, 8.0)
    return fresh.astype(jnp.bfloat16)


def draw_gain(key):
    return jax.random.uniform(key, (HEAD,), jnp.float32, 0.8, 1.6)


def draw_q_gain(key, part):
    return draw_gain(jax.random.fold_in(key, 303))


def draw_key_norm_gain(key, part):
    return draw_gain(jax.random.fold_in(key, 404))


def draw_text_mask(key, part):
    length = jax.random.randint(jax.random.fold_in(key, 505), (), TEXT // 8, TEXT + 1)
    return (jnp.arange(TEXT) < length).astype(jnp.int32)


def levels(rng, dims, cuts, low, high):
    def one(dim, shards_of):
        steps = jax.random.uniform(jax.random.fold_in(jax.random.fold_in(rng, 6), dim), (shards_of,), jnp.float32, low / len(cuts), high / len(cuts))
        return jnp.repeat(jnp.exp(steps), dims[dim] // shards_of).reshape((-1,) + (1,) * (len(dims) - dim - 1))

    loudness = one(*cuts[0])
    for cut in cuts[1:]:
        loudness = loudness * one(*cut)
    return loudness


def bell_draw(stream_key, shape, scale, limit, split=(), kind=jnp.bfloat16):
    loudness = levels(stream_key, shape, split, -0.22, 0.18) if split else 1.0
    values = jax.random.normal(stream_key, shape, jnp.float32) * scale * loudness
    return jnp.minimum(jnp.maximum(values, -limit), limit).astype(kind)


def setup_inputs(seed: int = 0, part: int = 0) -> dict:
    key_of = jax.random.split(jax.random.key(seed), 11)
    part_splits = jax.random.split(jax.random.fold_in(key_of[10], part), 11)
    visual_q = draw_visual_q(jax.random.fold_in(jax.random.fold_in(key_of[10], part), 71), part)
    visual_key_input = draw_visual_key_input(jax.random.fold_in(jax.random.fold_in(key_of[10], part), 71), part)
    visual_v = bell_draw(part_splits[2], (VIS, HEADS * HEAD), 1.0, 6.0, ((0, 32), (1, 2)))
    text_k = bell_draw(part_splits[3], (TEXT, HEADS * HEAD), 1.0, 6.0, ((0, 32), (1, 2)))
    text_v = bell_draw(part_splits[4], (TEXT, HEADS * HEAD), 1.0, 6.0, ((0, 32), (1, 2)))
    text_mask = draw_text_mask(jax.random.fold_in(jax.random.fold_in(key_of[10], part), 71), part)
    slab_order = jax.random.permutation(part_splits[6], N_SEQ).astype(jnp.int32)
    q_gain = draw_q_gain(jax.random.fold_in(key_of[10], 71), part)
    key_norm_gain = draw_key_norm_gain(jax.random.fold_in(key_of[10], 71), part)
    w_out = bell_draw(key_of[9], (HEADS * HEAD, D), 0.15, 0.8984375, ((0, 2),))
    return {"visual_q": visual_q, "visual_key_input": visual_key_input, "visual_v": visual_v, "text_k": text_k, "text_v": text_v, "text_mask": text_mask, "slab_order": slab_order, "q_gain": q_gain, "key_norm_gain": key_norm_gain, "w_out": w_out}


PARTS = (32, 48, 48)

def apply_norm(x, gain):
    x32 = x.astype(jnp.float32).reshape(x.shape[0], -1, 128)
    scale = lax.rsqrt(lax.optimization_barrier(jnp.mean(x32 * x32, axis=-1, keepdims=True)) + 0.05)
    return x32 * scale * gain

def angles(frame, height, column):
    pieces = []
    for pos, size in zip((frame, height, column), PARTS):
        half = size // 2
        freq = 10000.0 ** (-jnp.arange(half, dtype=jnp.float32) / half)
        pieces.append(pos.astype(jnp.float32)[:, None] * freq[None, :])
    angle = jnp.concatenate(pieces, axis=-1)
    return (jnp.cos(angle), jnp.sin(angle))

def apply_rotation(x, cosine_table, sine_table):
    outs = []
    offset = 0
    column = 0
    for size in PARTS:
        half = size // 2
        first = x[..., offset:offset + half]
        second = x[..., offset + half:offset + size]
        cpart = cosine_table[:, None, column:column + half]
        spart = sine_table[:, None, column:column + half]
        outs.append(first * cpart - second * spart)
        outs.append(second * cpart + first * spart)
        offset += size
        column += half
    return jnp.concatenate(outs, axis=-1)

def reference(visual_q, visual_key_input, visual_v, text_k, text_v, text_mask, slab_order, q_gain, key_norm_gain, w_out):
    index = jnp.arange(VIS, dtype=jnp.int32)
    owner = index // TOK_DEV
    local = index % TOK_DEV
    frame = local // (SLAB_H * WIDE)
    height = slab_order[owner] * SLAB_H + local // WIDE % SLAB_H
    column = local % WIDE
    cosine_table, sine_table = angles(frame, height, column)
    queries = (apply_rotation(apply_norm(visual_q, q_gain), cosine_table, sine_table) / jnp.sqrt(jnp.float32(HEAD))).astype(jnp.bfloat16)
    visual_key_rows = apply_rotation(apply_norm(visual_key_input, key_norm_gain), cosine_table, sine_table).astype(jnp.bfloat16)
    textual_keys = apply_norm(text_k, key_norm_gain).astype(jnp.bfloat16)
    key_rows = jnp.concatenate([visual_key_rows, textual_keys], axis=0).astype(jnp.float32)
    values = jnp.concatenate([visual_v, text_v], axis=0).reshape(VIS + TEXT, HEADS, HEAD).astype(jnp.float32)
    valid = jnp.concatenate([jnp.ones((VIS,), jnp.int32), text_mask.astype(jnp.int32)]) == 1
    blocks = queries.reshape(VIS // 256, 256, HEADS, HEAD) if VIS % 256 == 0 else queries.reshape(1, VIS, HEADS, HEAD)

    def attend(block):
        scores = jnp.einsum('qhd,khd->qhk', block.astype(jnp.float32), key_rows)
        scores = jnp.where(valid[None, None, :], scores, -jnp.inf)
        top = lax.optimization_barrier(jnp.max(scores, axis=-1, keepdims=True))
        probs = jnp.exp(scores - top)
        total = lax.optimization_barrier(jnp.sum(probs, axis=-1))
        weights = probs.astype(jnp.bfloat16).astype(jnp.float32)
        mixed = jnp.einsum('qhk,khd->qhd', weights, values)
        return (mixed / total[..., None]).astype(jnp.bfloat16)
    heads_out = lax.map(attend, blocks).reshape(VIS, HEADS * HEAD)
    group = HEADS * HEAD // N_TP
    summed = jnp.zeros((VIS, D), jnp.float32)
    for member in range(N_TP):
        partial_value = jnp.dot(heads_out[:, member * group:(member + 1) * group], w_out[member * group:(member + 1) * group, :], preferred_element_type=jnp.float32).astype(jnp.bfloat16)
        partial_value = lax.optimization_barrier(partial_value)
        summed = summed + partial_value.astype(jnp.float32)
    return summed.astype(jnp.bfloat16)
```

```python
import functools

import jax
import jax.numpy as jnp
import numpy as np
from jax import lax
from jax.experimental import pallas as pl
from jax.experimental.pallas import tpu as pltpu
from jax.sharding import PartitionSpec as P

SLAB_H = 2
WIDE = 32
SPLITS = (32, 48, 48)
HEAD = 128
NEGATIVE = -1e30
PAD = 8


def color_edges(edges, colors):
    at_src, at_dst = {}, {}
    for s, d in edges:
        at_src.setdefault(s, {})
        at_dst.setdefault(d, {})
    for s, d in edges:
        a = next(c for c in range(colors) if c not in at_src[s])
        b = next(c for c in range(colors) if c not in at_dst[d])
        if a != b:
            path = []
            node, side, want = d, 1, a
            while True:
                table = at_dst if side else at_src
                if want not in table[node]:
                    break
                other = table[node][want]
                path.append((other, node, want) if side else (node, other, want))
                node, side, want = other, 1 - side, (b if want == a else a)
            for ps, pd, c in path:
                del at_src[ps][c], at_dst[pd][c]
            for ps, pd, c in path:
                n = b if c == a else a
                at_src[ps][n] = pd
                at_dst[pd][n] = ps
        at_src[s][a] = d
        at_dst[d][a] = s
    return at_src


def plan(n_seq, n_tp, heads):
    total = heads * n_tp
    chips = 2
    rounds = n_seq // (chips * n_tp)
    owner = {}
    for arc in range(total):
        start = arc * n_seq // total
        tp, local = arc % n_tp, arc // n_tp
        seen = {}
        for z in range(n_seq):
            rel = (z - start - 1) % n_seq
            chip = (start + 1 if rel < n_seq // 2 else start) % n_seq
            count = seen.get(chip, 0)
            seen[chip] = count + 1
            owner[(z * n_tp + tp, local)] = chip * n_tp + count % n_tp
    edges = []
    for (src, local), dst in owner.items():
        edges.append((src, dst))
    colored = color_edges(sorted(edges), rounds)
    head_of = {(src, dst): local for (src, local), dst in owner.items()}
    perms = [[] for _ in range(rounds)]
    send = np.zeros((n_seq * n_tp, rounds), np.int32)
    valid = np.zeros((n_seq * n_tp, rounds), np.int32)
    for src, table in colored.items():
        for r, dst in table.items():
            perms[r].append((src, dst))
            send[src, r] = head_of[(src, dst)]
            valid[src, r] = 1
    cross, flip = [], []
    for arc in range(total):
        start = arc * n_seq // total
        after = (start + 1) % n_seq
        for t in range(n_tp):
            cross += [(start * n_tp + t, after * n_tp + t), (after * n_tp + t, start * n_tp + t)]
            flip += [(chip * n_tp + t, chip * n_tp + (t + 1) % n_tp) for chip in (start, after)]
    return rounds, [sorted(p) for p in perms], send, valid, cross, flip


def rope_tables(positions, size):
    half = size // 2
    freq = np.float32(10000.0) ** (-np.arange(half, dtype=np.float32) / np.float32(half))
    angle = np.asarray(positions, np.float32)[:, None] * freq[None, :]
    cos, sin = np.cos(angle), np.sin(angle)
    return np.concatenate([cos, cos], 1), np.concatenate([-sin, sin], 1)


def position_tables(rows, heights):
    local = np.arange(rows)
    parts = [
        rope_tables(local // (SLAB_H * WIDE), SPLITS[0]),
        rope_tables(np.zeros(rows), SPLITS[1]),
        rope_tables(local % WIDE, SPLITS[2]),
    ]
    tall = rope_tables(np.arange(heights), SPLITS[1])
    tall = [np.pad(t, ((0, 0), (SPLITS[0], SPLITS[2]))) for t in tall]
    fixed = [np.concatenate([p[i] for p in parts], 1) for i in range(2)]
    return [np.asarray(t, np.float32) for t in fixed + tall]


def prep_kernel(
    send_ref, mask_ref, slab_ref, q_ref, k_ref, v_ref, tk_ref, tv_ref, cos_ref, sin_ref, hcos_ref, hsin_ref, qg_ref, kg_ref,
    *outs, first,
):
    rows = q_ref.shape[0]
    texts = tk_ref.shape[0]
    here = lax.axis_index("seq") * lax.axis_size("tp") + lax.axis_index("tp")
    lane = lax.broadcasted_iota(jnp.int32, (rows, HEAD), 1)
    row = lax.broadcasted_iota(jnp.int32, (rows, HEAD), 0)
    in_first = lane < SPLITS[0]
    h0, h1 = SPLITS[0] // 2, SPLITS[1] // 2
    low = jnp.where(in_first, lane - h0, lax.rem(lane + SPLITS[1] - SPLITS[0], SPLITS[1]) - h1) < 0
    in_height = jnp.logical_and(lane >= SPLITS[0], lane < SPLITS[0] + SPLITS[1])
    which = lax.rem(lax.div(row, WIDE), SLAB_H)

    def table(fixed_ref, tall_ref):
        value = fixed_ref[...]
        for h in range(SLAB_H):
            mine = jnp.logical_and(in_height, which == h)
            value = jnp.where(mine, tall_ref[pl.ds(slab_ref[0] * SLAB_H + h, 1), :], value)
        return value

    cos = table(cos_ref, hcos_ref)
    sin = table(sin_ref, hsin_ref)
    marker = lax.broadcasted_iota(jnp.int32, (texts, HEAD), 0)
    marks = jnp.zeros((texts, HEAD), jnp.float32)
    for i in range(texts):
        marks = jnp.where(marker == i, mask_ref[i].astype(jnp.float32), marks)

    def norm(x, gain):
        x = x.astype(jnp.float32)
        return x * lax.rsqrt(jnp.mean(x * x, axis=-1, keepdims=True) + 0.05) * gain

    def rotate(x):
        up = jnp.where(in_first, pltpu.roll(x, HEAD - h0, 1), pltpu.roll(x, HEAD - h1, 1))
        down = jnp.where(in_first, pltpu.roll(x, h0, 1), pltpu.roll(x, h1, 1))
        return x * cos + jnp.where(low, up, down) * sin

    for r, out in enumerate(outs):
        col = pl.ds(pl.multiple_of(send_ref[here, first + r] * HEAD, HEAD), HEAD)
        q = rotate(norm(q_ref[:, col], qg_ref[...])) * np.float32(1.0 / np.sqrt(HEAD))
        out[0:rows, 0:HEAD] = q.astype(jnp.bfloat16)
        out[0:rows, HEAD : 2 * HEAD] = rotate(norm(k_ref[:, col], kg_ref[...])).astype(jnp.bfloat16)
        out[0:rows, 2 * HEAD :] = v_ref[:, col]
        tail = slice(rows, rows + texts + PAD)
        tk = norm(tk_ref[:, col], kg_ref[...])
        out[tail, 0:HEAD] = jnp.zeros((texts + PAD, HEAD), jnp.bfloat16)
        out[tail, HEAD : 2 * HEAD] = jnp.concatenate([tk, marks], axis=0).astype(jnp.bfloat16)
        tv = tv_ref[:, col].astype(jnp.float32)
        out[tail, 2 * HEAD :] = jnp.concatenate([tv, jnp.zeros_like(tv)], axis=0).astype(jnp.bfloat16)


def attention_kernel(*refs, tasks, chunks, rows, texts, q_tile):
    kv_refs, q_refs = refs[:chunks], refs[chunks : chunks + tasks]
    o_refs = refs[chunks + tasks : chunks + 2 * tasks]
    q_scr, o_scr, tk_scr, tv_scr = refs[chunks + 2 * tasks :]
    per = kv_refs[0].shape[0]
    tail = texts + PAD
    for r in range(tasks):
        q_scr[r * rows : (r + 1) * rows, :] = q_refs[r][0:rows, 0:HEAD]
    for c in range(chunks):
        for b in range(per):
            at = slice((c * per + b) * tail, (c * per + b + 1) * tail)
            tk_scr[at, :] = kv_refs[c][b, rows : rows + tail, 0:HEAD]
            tv_scr[at, :] = kv_refs[c][b, rows : rows + tail, HEAD:]
    n_text = chunks * per * tail
    marks = jnp.transpose(tk_scr[...].astype(jnp.float32))[0:1, :]
    marks = pltpu.roll(marks, n_text - texts, 1)
    lane = lax.broadcasted_iota(jnp.int32, (1, n_text), 1)
    bias = jnp.where((lane % tail < texts) & (marks > 0.5), 0.0, NEGATIVE)

    def step(state, q, k, v, extra):
        top, total, acc = state
        s = lax.dot_general(q, k, (((1,), (1,)), ((), ())), preferred_element_type=jnp.float32)
        if extra is not None:
            s = s + extra
        fresh = jnp.maximum(top, jnp.max(s, axis=-1, keepdims=True))
        p = jnp.exp(s - fresh)
        factor = jnp.exp(top - fresh)
        total = total * factor + jnp.sum(p, axis=-1, keepdims=True)
        acc = acc * factor + jnp.dot(p.astype(jnp.bfloat16), v, preferred_element_type=jnp.float32)
        return fresh, total, acc

    def tile(i, carry):
        at = pl.ds(pl.multiple_of(i * q_tile, q_tile), q_tile)
        q = q_scr[at, :]
        state = (
            jnp.full((q_tile, 1), NEGATIVE, jnp.float32),
            jnp.zeros((q_tile, 1), jnp.float32),
            jnp.zeros((q_tile, HEAD), jnp.float32),
        )
        for kv_ref in kv_refs:
            k = kv_ref[:, 0:rows, 0:HEAD].reshape(per * rows, HEAD)
            v = kv_ref[:, 0:rows, HEAD:].reshape(per * rows, HEAD)
            state = step(state, q, k, v, None)
        top, total, acc = step(state, q, tk_scr[...], tv_scr[...], bias)
        o_scr[at, :] = (acc / total).astype(jnp.bfloat16)
        return carry

    lax.fori_loop(0, tasks * rows // q_tile, tile, 0)
    for r in range(tasks):
        o_refs[r][...] = o_scr[r * rows : (r + 1) * rows, :]


def project_kernel(send_ref, valid_ref, w_ref, *refs, rounds):
    ins, (mine_ref, other_ref) = refs[:rounds], refs[rounds:]
    share = mine_ref.shape[0]
    me = lax.axis_index("tp")
    here = lax.axis_index("seq") * lax.axis_size("tp") + me
    rows = 2 * share
    width = w_ref.shape[0]
    heads = jnp.zeros((rows, HEAD), jnp.bfloat16)
    parts = []
    for j in range(width // HEAD):
        block = heads
        for r in range(rounds):
            hit = jnp.logical_and(send_ref[here, r] == j, valid_ref[here, r] == 1)
            block = jnp.where(hit, ins[r][...], block)
        parts.append(block)
    joined = jnp.concatenate(parts, axis=1)
    first = jnp.dot(joined, w_ref[...], preferred_element_type=jnp.float32).astype(jnp.bfloat16)
    low, high = first[:share], first[share:]
    mine_ref[...] = jnp.where(me == 0, low, high)
    other_ref[...] = jnp.where(me == 0, high, low)


def body(
    visual_q, visual_key_input, visual_v, text_k, text_v, text_mask, slab_order, q_gain, key_norm_gain, w_out
):
    rows, width = visual_q.shape
    texts = text_k.shape[0]
    heads = width // HEAD
    n_seq, n_tp = lax.axis_size("seq"), lax.axis_size("tp")
    rounds, perms, send, valid, cross, flip = plan(n_seq, n_tp, heads)
    both = ("seq", "tp")
    full = rows + texts + PAD
    vmem = pl.BlockSpec(memory_space=pltpu.VMEM)
    smem = pl.BlockSpec(memory_space=pltpu.SMEM)
    tables = position_tables(rows, n_seq * SLAB_H)
    half = rounds // 2
    got, chunks = [], []
    for first in (0, half):
        blocks = pl.pallas_call(
            functools.partial(prep_kernel, first=first),
            out_shape=[jax.ShapeDtypeStruct((full, 3 * HEAD), jnp.bfloat16)] * half,
            in_specs=[smem] * 3 + [vmem] * 11,
            out_specs=[vmem] * half,
            name="prep",
        )(
            send, text_mask, slab_order, visual_q, visual_key_input, visual_v, text_k, text_v, *tables,
            q_gain.reshape(1, HEAD), key_norm_gain.reshape(1, HEAD),
        )
        got += [lax.ppermute(b, both, perms[first + r]) for r, b in enumerate(blocks)]
    for first in (0, half):
        own = jnp.stack([g[:, HEAD:] for g in got[first : first + half]])
        across = lax.ppermute(own, both, cross)
        chunks += [own, across, lax.ppermute(own, both, flip), lax.ppermute(across, both, flip)]
    n_text = n_seq * (texts + PAD)
    outs = []
    for first in (0, half):
        outs += pl.pallas_call(
            functools.partial(
                attention_kernel, tasks=half, chunks=len(chunks), rows=rows, texts=texts, q_tile=2 * rows
            ),
            out_shape=[jax.ShapeDtypeStruct((rows, HEAD), jnp.bfloat16)] * half,
            in_specs=[vmem] * (len(chunks) + half),
            out_specs=[vmem] * half,
            scratch_shapes=[
                pltpu.VMEM((half * rows, HEAD), jnp.bfloat16),
                pltpu.VMEM((half * rows, HEAD), jnp.bfloat16),
                pltpu.VMEM((n_text, HEAD), jnp.bfloat16),
                pltpu.VMEM((n_text, HEAD), jnp.bfloat16),
            ],
            name="attention",
        )(*chunks, *got[first : first + half])
    back = [lax.ppermute(o, both, [(d, s) for s, d in p]) for o, p in zip(outs, perms)]
    share = rows // n_tp
    mine, other = pl.pallas_call(
        functools.partial(project_kernel, rounds=rounds),
        out_shape=[jax.ShapeDtypeStruct((share, w_out.shape[1]), jnp.bfloat16)] * 2,
        in_specs=[smem] * 2 + [vmem] * (1 + rounds),
        out_specs=[vmem] * 2,
        name="project",
    )(send, valid, w_out, *back)
    theirs = lax.ppermute(other, "tp", [(0, 1), (1, 0)])
    return (mine.astype(jnp.float32) + theirs.astype(jnp.float32)).astype(jnp.bfloat16)


def solution(mesh):
    wide = P(("grp", "seq"), "tp")
    long = P(("grp", "seq"))
    placed = (wide, wide, wide, wide, wide, long, long, P(), P(), P("tp", None))
    return jax.shard_map(
        body, mesh=mesh, in_specs=placed, out_specs=P(("grp", "seq", "tp"), None), check_vma=False
    )
```

```python
import functools

import jax
import jax.numpy as jnp
import numpy as np
from jax import lax
from jax.experimental import pallas as pl
from jax.experimental.pallas import tpu as pltpu
from jax.sharding import PartitionSpec as P


SLAB_H = 2
WIDE = 32
SPLITS = (32, 48, 48)
HEAD = 128
NEGATIVE = -1e30
PAD = 8


def color_edges(edges, colors):
    at_src, at_dst = {}, {}
    for s, d in edges:
        at_src.setdefault(s, {})
        at_dst.setdefault(d, {})
    for s, d in edges:
        a = next(c for c in range(colors) if c not in at_src[s])
        b = next(c for c in range(colors) if c not in at_dst[d])
        if a != b:
            path = []
            node, side, want = d, 1, a
            while True:
                table = at_dst if side else at_src
                if want not in table[node]:
                    break
                other = table[node][want]
                path.append((other, node, want) if side else (node, other, want))
                node, side, want = other, 1 - side, (b if want == a else a)
            for ps, pd, c in path:
                del at_src[ps][c], at_dst[pd][c]
            for ps, pd, c in path:
                n = b if c == a else a
                at_src[ps][n] = pd
                at_dst[pd][n] = ps
        at_src[s][a] = d
        at_dst[d][a] = s
    return at_src


def sort_rounds(at_src, at_dst, colors, n_tp, cost):
    for _ in range(20):
        moved = False
        for a in range(colors):
            for b in range(a + 1, colors):
                seen = set()
                ends = [(0, n) for n in at_src if (a in at_src[n]) != (b in at_src[n])]
                ends += [(1, n) for n in at_dst if (a in at_dst[n]) != (b in at_dst[n])]
                ends += [(0, n) for n in at_src if a in at_src[n]]
                for start in ends:
                    stack, edges = [start], set()
                    while stack:
                        side, n = stack.pop()
                        if (side, n) in seen:
                            continue
                        seen.add((side, n))
                        table = (at_dst if side else at_src)[n]
                        for c in (a, b):
                            if c in table:
                                edges.add((table[c], n, c) if side else (n, table[c], c))
                                stack.append((1 - side, table[c]))
                    gain = sum(cost(s, d, c) - cost(s, d, a + b - c) for s, d, c in edges)
                    if gain > 1e-6:
                        moved = True
                        for s, d, c in edges:
                            del at_src[s][c], at_dst[d][c]
                        for s, d, c in edges:
                            at_src[s][a + b - c] = d
                            at_dst[d][a + b - c] = s
        for chip in sorted({d // n_tp for d in at_dst}):
            slots = [(d, r) for d in sorted(at_dst) if d // n_tp == chip for r in range(colors)]
            for i in range(len(slots)):
                for j in range(i):
                    (d1, r1), (d2, r2) = slots[i], slots[j]
                    s1, s2 = at_dst[d1][r1], at_dst[d2][r2]
                    if r1 == r2 or s1 == s2 or r2 in at_src[s1] or r1 in at_src[s2]:
                        continue
                    before = cost(s1, d1, r1) + cost(s2, d2, r2)
                    if cost(s1, d2, r2) + cost(s2, d1, r1) < before - 1e-6:
                        moved = True
                        del at_src[s1][r1], at_src[s2][r2]
                        at_src[s1][r2], at_src[s2][r1] = d2, d1
                        at_dst[d1][r1], at_dst[d2][r2] = s2, s1
        if not moved:
            break


def plan(n_seq, n_tp, heads):
    total = heads * n_tp
    chips = 2
    rounds = n_seq // (chips * n_tp)
    owner = {}
    for arc in range(total):
        start = arc * n_seq // total
        tp, local = arc % n_tp, arc // n_tp
        for z in range(n_seq):
            rel = (z - start - 1) % n_seq
            near, chip = (rel, start + 1) if rel < n_seq // 2 else (n_seq - 1 - rel, start)
            owner[(z * n_tp + tp, local)] = chip % n_seq * n_tp + near % n_tp
    at_src = color_edges(sorted((src, dst) for (src, _), dst in owner.items()), rounds)
    at_dst = {}
    for src, table in at_src.items():
        for r, dst in table.items():
            at_dst.setdefault(dst, {})[r] = src

    def hops(src, dst):
        apart = abs(src // n_tp - dst // n_tp)
        return min(apart, n_seq - apart)

    per_round = n_seq / 2 / rounds
    for power in (1, 2, 3, 4):
        sort_rounds(
            at_src, at_dst, rounds, n_tp, lambda s, d, c: abs(hops(s, d) - per_round * (c + 0.25)) ** power
        )
    order = [r for pair in zip(reversed(range(rounds // 2, rounds)), range(rounds // 2)) for r in pair]
    local_of = {}
    for (src, local), dst in owner.items():
        local_of.setdefault((src, dst // n_tp), []).append(local)
    perms = [[] for _ in range(rounds)]
    send = np.zeros((n_seq * n_tp, rounds), np.int32)
    valid = np.zeros((n_seq * n_tp, rounds), np.int32)
    for src in sorted(at_src):
        for r, dst in sorted(at_src[src].items()):
            (local,) = local_of[(src, dst // n_tp)]
            slot = order.index(r)
            perms[slot].append((src, dst))
            send[src, slot] = local
            valid[src, slot] = 1
    cross, flip = [], []
    for arc in range(total):
        start = arc * n_seq // total
        after = (start + 1) % n_seq
        for t in range(n_tp):
            cross += [(start * n_tp + t, after * n_tp + t), (after * n_tp + t, start * n_tp + t)]
            flip += [(chip * n_tp + t, chip * n_tp + (t + 1) % n_tp) for chip in (start, after)]
    return rounds, perms, send, valid, cross, flip


def rope_tables(positions, size):
    half = size // 2
    freq = np.float32(10000.0) ** (-np.arange(half, dtype=np.float32) / np.float32(half))
    angle = np.asarray(positions, np.float32)[:, None] * freq[None, :]
    cos, sin = np.cos(angle), np.sin(angle)
    return np.concatenate([cos, cos], 1), np.concatenate([-sin, sin], 1)


def position_tables(rows, heights):
    local = np.arange(rows)
    parts = [
        rope_tables(local // (SLAB_H * WIDE), SPLITS[0]),
        rope_tables(np.zeros(rows), SPLITS[1]),
        rope_tables(local % WIDE, SPLITS[2]),
    ]
    tall = rope_tables(np.arange(heights), SPLITS[1])
    tall = [np.pad(t, ((0, 0), (SPLITS[0], SPLITS[2]))) for t in tall]
    fixed = [np.concatenate([p[i] for p in parts], 1) for i in range(2)]
    return [np.asarray(t, np.float32) for t in fixed + tall]


def prep_kernel(
    send_ref, mask_ref, slab_ref, q_ref, k_ref, v_ref, tk_ref, tv_ref, cos_ref, sin_ref, hcos_ref, hsin_ref, qg_ref, kg_ref,
    *outs, first,
):
    rows = q_ref.shape[0]
    texts = tk_ref.shape[0]
    here = lax.axis_index("seq") * lax.axis_size("tp") + lax.axis_index("tp")
    lane = lax.broadcasted_iota(jnp.int32, (rows, HEAD), 1)
    row = lax.broadcasted_iota(jnp.int32, (rows, HEAD), 0)
    in_first = lane < SPLITS[0]
    h0, h1 = SPLITS[0] // 2, SPLITS[1] // 2
    low = jnp.where(in_first, lane - h0, lax.rem(lane + SPLITS[1] - SPLITS[0], SPLITS[1]) - h1) < 0
    in_height = jnp.logical_and(lane >= SPLITS[0], lane < SPLITS[0] + SPLITS[1])
    which = lax.rem(lax.div(row, WIDE), SLAB_H)

    def table(fixed_ref, tall_ref):
        value = fixed_ref[...]
        for h in range(SLAB_H):
            mine = jnp.logical_and(in_height, which == h)
            value = jnp.where(mine, tall_ref[pl.ds(slab_ref[0] * SLAB_H + h, 1), :], value)
        return value

    cos = table(cos_ref, hcos_ref)
    sin = table(sin_ref, hsin_ref)
    marker = lax.broadcasted_iota(jnp.int32, (texts, HEAD), 0)
    marks = jnp.zeros((texts, HEAD), jnp.float32)
    for i in range(texts):
        marks = jnp.where(marker == i, mask_ref[i].astype(jnp.float32), marks)

    def norm(x, gain):
        x = x.astype(jnp.float32)
        return x * lax.rsqrt(jnp.mean(x * x, axis=-1, keepdims=True) + 0.05) * gain

    def rotate(x):
        up = jnp.where(in_first, pltpu.roll(x, HEAD - h0, 1), pltpu.roll(x, HEAD - h1, 1))
        down = jnp.where(in_first, pltpu.roll(x, h0, 1), pltpu.roll(x, h1, 1))
        return x * cos + jnp.where(low, up, down) * sin

    for r, out in enumerate(outs):
        col = pl.ds(pl.multiple_of(send_ref[here, first + r] * HEAD, HEAD), HEAD)
        q = rotate(norm(q_ref[:, col], qg_ref[...])) * np.float32(1.0 / np.sqrt(HEAD))
        out[0:rows, 0:HEAD] = q.astype(jnp.bfloat16)
        out[0:rows, HEAD : 2 * HEAD] = rotate(norm(k_ref[:, col], kg_ref[...])).astype(jnp.bfloat16)
        out[0:rows, 2 * HEAD :] = v_ref[:, col]
        tail = slice(rows, rows + texts)
        out[tail, 0:HEAD] = marks.astype(jnp.bfloat16)
        out[tail, HEAD : 2 * HEAD] = norm(tk_ref[:, col], kg_ref[...]).astype(jnp.bfloat16)
        out[tail, 2 * HEAD :] = tv_ref[:, col]


def pack_kernel(*refs):
    *ins, out = refs
    rows = out.shape[1] - PAD
    visual = ins[0].shape[0] - PAD
    for b, ref in enumerate(ins):
        out[b, 0:visual, :] = ref[0:visual, HEAD:]
        text = ref[visual:rows, HEAD:]
        marks = ref[visual:rows, 0:HEAD]
        marks = jnp.concatenate([marks, marks], axis=1)
        out[b, visual:, :] = jnp.concatenate([text.astype(jnp.float32), marks.astype(jnp.float32)], axis=0).astype(
            jnp.bfloat16
        )


def attention_kernel(*refs, tasks, chunks, rows, texts, q_tile, k_blocks, final):
    refs = list(refs)

    def take(n):
        head, refs[:] = refs[:n], refs[n:]
        return head

    kv_refs, q_refs = take(chunks), take(tasks)
    state_in = take(3) if final else None
    outs = take(tasks) if final else take(3)
    q_scr, o_scr, tk_scr, tv_scr = refs
    per = kv_refs[0].shape[0]
    tail = texts + PAD
    for r in range(tasks):
        q_scr[r * rows : (r + 1) * rows, :] = q_refs[r][0:rows, 0:HEAD]
    for c in range(chunks):
        for b in range(per):
            at = slice((c * per + b) * tail, (c * per + b + 1) * tail)
            tk_scr[at, :] = kv_refs[c][b, rows : rows + tail, 0:HEAD]
            tv_scr[at, :] = kv_refs[c][b, rows : rows + tail, HEAD:]
    n_text = chunks * per * tail
    marks = jnp.transpose(tk_scr[...].astype(jnp.float32))[0:1, :]
    marks = pltpu.roll(marks, n_text - texts, 1)
    lane = lax.broadcasted_iota(jnp.int32, (1, n_text), 1)
    bias = jnp.where((lane % tail < texts) & (marks > 0.5), 0.0, NEGATIVE)

    def score(q, k):
        return lax.dot_general(q, k, (((1,), (1,)), ((), ())), preferred_element_type=jnp.float32)

    def absorb(state, s, v):
        top, total, acc = state
        fresh = jnp.maximum(top, jnp.max(s, axis=-1, keepdims=True))
        p = jnp.exp(s - fresh)
        factor = jnp.exp(top - fresh)
        total = total * factor + jnp.sum(p, axis=-1, keepdims=True)
        acc = acc * factor + jnp.dot(p.astype(jnp.bfloat16), v, preferred_element_type=jnp.float32)
        return fresh, total, acc

    def tile(i, carry):
        at = pl.ds(pl.multiple_of(i * q_tile, q_tile), q_tile)
        q = q_scr[at, :]
        state = (
            jnp.full((q_tile, 1), NEGATIVE, jnp.float32),
            jnp.zeros((q_tile, 1), jnp.float32),
            jnp.zeros((q_tile, HEAD), jnp.float32),
        )
        spans = [(ref, slice(b, b + k_blocks)) for ref in kv_refs for b in range(0, per, k_blocks)]
        ready = score(q, tk_scr[...]) + bias
        value = tv_scr[...]
        for ref, at_b in spans:
            ahead = score(q, ref[at_b, 0:rows, 0:HEAD].reshape(k_blocks * rows, HEAD))
            state = absorb(state, ready, value)
            ready, value = ahead, ref[at_b, 0:rows, HEAD:].reshape(k_blocks * rows, HEAD)
        top, total, acc = absorb(state, ready, value)
        top = jnp.broadcast_to(top, (q_tile, HEAD))
        total = jnp.broadcast_to(total, (q_tile, HEAD))
        if final:
            top_in, total_in, acc_in = (ref[at, :] for ref in state_in)
            high = jnp.maximum(top, top_in)
            here, there = jnp.exp(top - high), jnp.exp(top_in - high)
            acc = acc * here + acc_in * there
            o_scr[at, :] = (acc / (total * here + total_in * there)).astype(jnp.bfloat16)
        else:
            outs[0][at, :] = top
            outs[1][at, :] = total
            outs[2][at, :] = acc
        return carry

    lax.fori_loop(0, tasks * rows // q_tile, tile, 0)
    if final:
        for r in range(tasks):
            outs[r][...] = o_scr[r * rows : (r + 1) * rows, :]


def attend(chunks, queries, state, rows, texts, final):
    tasks = len(queries)
    vmem = pl.BlockSpec(memory_space=pltpu.VMEM)
    many = tasks * rows
    n_text = sum(c.shape[0] for c in chunks) * (texts + PAD)
    if final:
        shapes = [jax.ShapeDtypeStruct((rows, HEAD), jnp.bfloat16)] * tasks
    else:
        shapes = [jax.ShapeDtypeStruct((many, HEAD), jnp.float32)] * 3
    extra = [] if state is None else list(state)
    return pl.pallas_call(
        functools.partial(
            attention_kernel, tasks=tasks, chunks=len(chunks), rows=rows, texts=texts, q_tile=2 * rows,
            k_blocks=tasks // 2, final=final,
        ),
        out_shape=shapes,
        in_specs=[vmem] * (len(chunks) + tasks + len(extra)),
        out_specs=[vmem] * len(shapes),
        scratch_shapes=[
            pltpu.VMEM((many, HEAD), jnp.bfloat16),
            pltpu.VMEM((many, HEAD), jnp.bfloat16),
            pltpu.VMEM((n_text, HEAD), jnp.bfloat16),
            pltpu.VMEM((n_text, HEAD), jnp.bfloat16),
        ],
        name="attention",
    )(*chunks, *queries, *extra)


def project_kernel(send_ref, valid_ref, w_ref, *refs, rounds):
    ins, (mine_ref, other_ref, joined) = refs[:rounds], refs[rounds:]
    share = mine_ref.shape[0]
    me = lax.axis_index("tp")
    here = lax.axis_index("seq") * lax.axis_size("tp") + me

    for r in range(rounds):

        @pl.when(valid_ref[here, r] == 1)
        def _():
            at = pl.ds(pl.multiple_of(send_ref[here, r] * HEAD, HEAD), HEAD)
            joined[:, at] = ins[r][...]

    first = jnp.dot(joined[...], w_ref[...], preferred_element_type=jnp.float32).astype(jnp.bfloat16)
    low, high = first[:share], first[share:]
    mine_ref[...] = jnp.where(me == 0, low, high)
    other_ref[...] = jnp.where(me == 0, high, low)


def body(
    visual_q, visual_key_input, visual_v, text_k, text_v, text_mask, slab_order, q_gain, key_norm_gain, w_out
):
    rows, width = visual_q.shape
    texts = text_k.shape[0]
    heads = width // HEAD
    n_seq, n_tp = lax.axis_size("seq"), lax.axis_size("tp")
    rounds, perms, send, valid, cross, flip = plan(n_seq, n_tp, heads)
    both = ("seq", "tp")
    full = rows + texts
    vmem = pl.BlockSpec(memory_space=pltpu.VMEM)
    smem = pl.BlockSpec(memory_space=pltpu.SMEM)
    tables = position_tables(rows, n_seq * SLAB_H)
    half = rounds // 2
    got = []
    for first in (0, half):
        blocks = pl.pallas_call(
            functools.partial(prep_kernel, first=first),
            out_shape=[jax.ShapeDtypeStruct((full, 3 * HEAD), jnp.bfloat16)] * half,
            in_specs=[smem] * 3 + [vmem] * 11,
            out_specs=[vmem] * half,
            name="prep",
        )(
            send, text_mask, slab_order, visual_q, visual_key_input, visual_v, text_k, text_v, *tables,
            q_gain.reshape(1, HEAD), key_norm_gain.reshape(1, HEAD),
        )
        for r, b in enumerate(blocks, first):
            got.append(lax.ppermute(b, both, perms[r]))
    own = pl.pallas_call(
        pack_kernel,
        out_shape=jax.ShapeDtypeStruct((rounds, full + PAD, 2 * HEAD), jnp.bfloat16),
        in_specs=[vmem] * rounds,
        out_specs=vmem,
        name="pack",
    )(*got)
    across = lax.ppermute(own, both, cross)
    peer = lax.ppermute(own, both, flip)
    state = attend([own, peer], got, None, rows, texts, False)
    peer_across = lax.ppermute(across, both, flip)
    outs = attend([across, peer_across], got, state, rows, texts, True)
    back = [None] * rounds
    for r in range(rounds):
        back[r] = lax.ppermute(outs[r], both, [(d, s) for s, d in perms[r]])
    share = rows // n_tp
    mine, other = pl.pallas_call(
        functools.partial(project_kernel, rounds=rounds),
        out_shape=[jax.ShapeDtypeStruct((share, w_out.shape[1]), jnp.bfloat16)] * 2,
        in_specs=[smem] * 2 + [vmem] * (1 + rounds),
        out_specs=[vmem] * 2,
        scratch_shapes=[pltpu.VMEM((rows, width), jnp.bfloat16)],
        name="project",
    )(send, valid, w_out, *back)
    theirs = lax.ppermute(other, "tp", [(0, 1), (1, 0)])
    return (mine.astype(jnp.float32) + theirs.astype(jnp.float32)).astype(jnp.bfloat16)


def solution(mesh):
    wide = P(("grp", "seq"), "tp")
    long = P(("grp", "seq"))
    placed = (wide, wide, wide, wide, wide, long, long, P(), P(), P("tp", None))
    return jax.shard_map(body, mesh=mesh, in_specs=placed, out_specs=P(("grp", "seq", "tp"), None), check_vma=False)
```

```python
import functools

import jax
import jax.numpy as jnp
import numpy as np
from jax import lax
from jax.experimental import pallas as pl
from jax.experimental.pallas import tpu as pltpu
from jax.sharding import PartitionSpec as P


SLAB_H = 2
WIDE = 32
SPLITS = (32, 48, 48)
HEAD = 128
NEGATIVE = -1e30
PAD = 8


def color_edges(edges, colors):
    at_src, at_dst = {}, {}
    for s, d in edges:
        at_src.setdefault(s, {})
        at_dst.setdefault(d, {})
    for s, d in edges:
        a = next(c for c in range(colors) if c not in at_src[s])
        b = next(c for c in range(colors) if c not in at_dst[d])
        if a != b:
            path = []
            node, side, want = d, 1, a
            while True:
                table = at_dst if side else at_src
                if want not in table[node]:
                    break
                other = table[node][want]
                path.append((other, node, want) if side else (node, other, want))
                node, side, want = other, 1 - side, (b if want == a else a)
            for ps, pd, c in path:
                del at_src[ps][c], at_dst[pd][c]
            for ps, pd, c in path:
                n = b if c == a else a
                at_src[ps][n] = pd
                at_dst[pd][n] = ps
        at_src[s][a] = d
        at_dst[d][a] = s
    return at_src


def sort_rounds(at_src, at_dst, colors, cost):
    for _ in range(20):
        moved = False
        for a in range(colors):
            for b in range(a + 1, colors):
                seen = set()
                ends = [(0, n) for n in at_src if (a in at_src[n]) != (b in at_src[n])]
                ends += [(1, n) for n in at_dst if (a in at_dst[n]) != (b in at_dst[n])]
                ends += [(0, n) for n in at_src if a in at_src[n]]
                for start in ends:
                    stack, edges = [start], set()
                    while stack:
                        side, n = stack.pop()
                        if (side, n) in seen:
                            continue
                        seen.add((side, n))
                        table = (at_dst if side else at_src)[n]
                        for c in (a, b):
                            if c in table:
                                edges.add((table[c], n, c) if side else (n, table[c], c))
                                stack.append((1 - side, table[c]))
                    gain = sum(cost(s, d, c) - cost(s, d, a + b - c) for s, d, c in edges)
                    if gain > 1e-6:
                        moved = True
                        for s, d, c in edges:
                            del at_src[s][c], at_dst[d][c]
                        for s, d, c in edges:
                            at_src[s][a + b - c] = d
                            at_dst[d][a + b - c] = s
        if not moved:
            break


def plan(n_seq, n_tp, heads):
    total = heads * n_tp
    chips = 2
    rounds = n_seq // (chips * n_tp)
    backs = rounds // 2
    owner, local_of, back_edges, task_of, swap = {}, {}, [], {}, []
    for pair in range(total // 2):
        tp = pair % n_tp
        starts = [arc * n_seq // total for arc in (2 * pair, 2 * pair + 1)]
        middle = (starts[0] + starts[1] + 2) // 2
        for z in range(n_seq):
            rel = (z - middle) % n_seq
            near, right = (rel, 1) if rel < n_seq // 2 else (n_seq - 1 - rel, 0)
            src = z * n_tp + tp
            devices = [(start + right) % n_seq * n_tp + near % n_tp for start in starts]
            for side in range(2):
                local = pair // n_tp * 2 + side
                owner[(src, local)] = devices[side]
                local_of[(src, devices[side])] = local
            keep = right ^ (near < n_seq // 4)
            back_edges.append((src, devices[keep]))
            task_of[(src, devices[keep])] = devices[1 - keep]
            if near < n_tp:
                swap += [tuple(devices), tuple(reversed(devices))]

    def hops(src, dst):
        apart = abs(src // n_tp - dst // n_tp)
        return min(apart, n_seq - apart)

    def sorted_rounds(edges, colors):
        at_src = color_edges(sorted(edges), colors)
        at_dst = {}
        for src, table in at_src.items():
            for r, dst in table.items():
                at_dst.setdefault(dst, {})[r] = src
        per_round = n_seq / 2 / colors
        for power in (1, 2, 3, 4):
            sort_rounds(
                at_src, at_dst, colors, lambda s, d, c: abs(hops(s, d) - per_round * (c + 0.25)) ** power
            )
        return at_src

    order = [r for pair in zip(reversed(range(rounds // 2, rounds)), range(rounds // 2)) for r in pair]
    perms = [[] for _ in range(rounds)]
    send = np.zeros((n_seq * n_tp, rounds), np.int32)
    slot_of = {}
    for src, table in sorted(sorted_rounds([(s, d) for (s, _), d in owner.items()], rounds).items()):
        for r, dst in sorted(table.items()):
            slot = order.index(r)
            perms[slot].append((src, dst))
            send[src, slot] = local_of[(src, dst)]
            slot_of[(src, dst)] = slot
    perms_back = [[] for _ in range(backs)]
    place = np.tile(np.arange(rounds, dtype=np.int32), (n_seq * n_tp, 1))
    heads_back = np.zeros((n_seq * n_tp, 2 * backs), np.int32)
    valid = np.zeros((n_seq * n_tp, backs), np.int32)
    for src, table in sorted(sorted_rounds(back_edges, backs).items()):
        for r, dst in sorted(table.items()):
            j = backs - 1 - r
            other = task_of[(src, dst)]
            perms_back[j].append((dst, src))
            place[dst, slot_of[(src, dst)]] = backs + j
            place[other, slot_of[(src, other)]] = j
            heads_back[src, 2 * j] = local_of[(src, dst)]
            heads_back[src, 2 * j + 1] = local_of[(src, other)]
            valid[src, j] = 1
    cross, flip = [], []
    for arc in range(total):
        start = arc * n_seq // total
        after = (start + 1) % n_seq
        for t in range(n_tp):
            cross += [(start * n_tp + t, after * n_tp + t), (after * n_tp + t, start * n_tp + t)]
            flip += [(chip * n_tp + t, chip * n_tp + (t + 1) % n_tp) for chip in (start, after)]
    return perms, send, cross, flip, place, sorted(set(swap)), perms_back, heads_back, valid


def rope_tables(positions, size):
    half = size // 2
    freq = np.float32(10000.0) ** (-np.arange(half, dtype=np.float32) / np.float32(half))
    angle = np.asarray(positions, np.float32)[:, None] * freq[None, :]
    cos, sin = np.cos(angle), np.sin(angle)
    return np.concatenate([cos, cos], 1), np.concatenate([-sin, sin], 1)


def position_tables(rows, heights):
    local = np.arange(rows)
    parts = [
        rope_tables(local // (SLAB_H * WIDE), SPLITS[0]),
        rope_tables(np.zeros(rows), SPLITS[1]),
        rope_tables(local % WIDE, SPLITS[2]),
    ]
    tall = rope_tables(np.arange(heights), SPLITS[1])
    tall = [np.pad(t, ((0, 0), (SPLITS[0], SPLITS[2]))) for t in tall]
    fixed = [np.concatenate([p[i] for p in parts], 1) for i in range(2)]
    return [np.asarray(t, np.float32) for t in fixed + tall]


def prep_kernel(
    send_ref, mask_ref, slab_ref, q_ref, k_ref, v_ref, tk_ref, tv_ref, cos_ref, sin_ref, hcos_ref, hsin_ref, qg_ref, kg_ref,
    *outs, first,
):
    rows = q_ref.shape[0]
    texts = tk_ref.shape[0]
    here = lax.axis_index("seq") * lax.axis_size("tp") + lax.axis_index("tp")
    lane = lax.broadcasted_iota(jnp.int32, (rows, HEAD), 1)
    row = lax.broadcasted_iota(jnp.int32, (rows, HEAD), 0)
    in_first = lane < SPLITS[0]
    h0, h1 = SPLITS[0] // 2, SPLITS[1] // 2
    low = jnp.where(in_first, lane - h0, lax.rem(lane + SPLITS[1] - SPLITS[0], SPLITS[1]) - h1) < 0
    in_height = jnp.logical_and(lane >= SPLITS[0], lane < SPLITS[0] + SPLITS[1])
    which = lax.rem(lax.div(row, WIDE), SLAB_H)

    def table(fixed_ref, tall_ref):
        value = fixed_ref[...]
        for h in range(SLAB_H):
            mine = jnp.logical_and(in_height, which == h)
            value = jnp.where(mine, tall_ref[pl.ds(slab_ref[0] * SLAB_H + h, 1), :], value)
        return value

    cos = table(cos_ref, hcos_ref)
    sin = table(sin_ref, hsin_ref)
    marker = lax.broadcasted_iota(jnp.int32, (texts, HEAD), 0)
    marks = jnp.zeros((texts, HEAD), jnp.float32)
    for i in range(texts):
        marks = jnp.where(marker == i, mask_ref[i].astype(jnp.float32), marks)

    def norm(x, gain):
        x = x.astype(jnp.float32)
        return x * lax.rsqrt(jnp.mean(x * x, axis=-1, keepdims=True) + 0.05) * gain

    def rotate(x):
        up = jnp.where(in_first, pltpu.roll(x, HEAD - h0, 1), pltpu.roll(x, HEAD - h1, 1))
        down = jnp.where(in_first, pltpu.roll(x, h0, 1), pltpu.roll(x, h1, 1))
        return x * cos + jnp.where(low, up, down) * sin

    for r, out in enumerate(outs):
        col = pl.ds(pl.multiple_of(send_ref[here, first + r] * HEAD, HEAD), HEAD)
        q = rotate(norm(q_ref[:, col], qg_ref[...])) * np.float32(1.0 / np.sqrt(HEAD))
        out[0:rows, 0:HEAD] = q.astype(jnp.bfloat16)
        out[0:rows, HEAD : 2 * HEAD] = rotate(norm(k_ref[:, col], kg_ref[...])).astype(jnp.bfloat16)
        out[0:rows, 2 * HEAD :] = v_ref[:, col]
        tail = slice(rows, rows + texts)
        out[tail, 0:HEAD] = marks.astype(jnp.bfloat16)
        out[tail, HEAD : 2 * HEAD] = norm(tk_ref[:, col], kg_ref[...]).astype(jnp.bfloat16)
        out[tail, 2 * HEAD :] = tv_ref[:, col]


def pack_kernel(*refs):
    *ins, out = refs
    rows = out.shape[1] - PAD
    visual = ins[0].shape[0] - PAD
    for b, ref in enumerate(ins):
        out[b, 0:visual, :] = ref[0:visual, HEAD:]
        text = ref[visual:rows, HEAD:]
        marks = ref[visual:rows, 0:HEAD]
        marks = jnp.concatenate([marks, marks], axis=1)
        out[b, visual:, :] = jnp.concatenate([text.astype(jnp.float32), marks.astype(jnp.float32)], axis=0).astype(
            jnp.bfloat16
        )


def attend(q_ref, kv_refs, tk_scr, v_scr, rows, texts, q_tile, k_blocks, finish):
    per = kv_refs[0].shape[0]
    tail = texts + PAD
    for c, ref in enumerate(kv_refs):
        for b in range(per):
            at = slice((c * per + b) * tail, (c * per + b + 1) * tail)
            tk_scr[at, :] = ref[b, rows : rows + tail, 0:HEAD]
            v_scr[at, 0:HEAD] = ref[b, rows : rows + tail, HEAD:]
            v_at = (c * per + b) * rows + len(kv_refs) * per * tail
            v_scr[v_at : v_at + rows, 0:HEAD] = ref[b, 0:rows, HEAD:]
    v_scr[:, HEAD:] = jnp.ones((v_scr.shape[0], HEAD), jnp.bfloat16)
    n_text = len(kv_refs) * per * tail
    marks = jnp.transpose(tk_scr[...].astype(jnp.float32))[0:1, :]
    marks = pltpu.roll(marks, n_text - texts, 1)
    lane = lax.broadcasted_iota(jnp.int32, (1, n_text), 1)
    bias = jnp.where((lane % tail < texts) & (marks > 0.5), 0.0, NEGATIVE)

    def score(q, k):
        return lax.dot_general(q, k, (((1,), (1,)), ((), ())), preferred_element_type=jnp.float32)

    def absorb(state, s, v):
        top, acc = state
        fresh = jnp.maximum(top, jnp.max(s, axis=-1, keepdims=True))
        p = jnp.exp(s - fresh)
        factor = jnp.exp(top - fresh)
        acc = acc * factor + jnp.dot(p.astype(jnp.bfloat16), v, preferred_element_type=jnp.float32)
        return fresh, acc

    def tile(i, carry):
        at = pl.ds(pl.multiple_of(i * q_tile, q_tile), q_tile)
        q = q_ref[at, :]
        state = (
            jnp.full((q_tile, 1), NEGATIVE, jnp.float32),
            jnp.zeros((q_tile, 2 * HEAD), jnp.float32),
        )
        spans = [(ref, slice(b, b + k_blocks)) for ref in kv_refs for b in range(0, per, k_blocks)]
        ready = score(q, tk_scr[...]) + bias
        value = v_scr[0:n_text, :]
        for n, (ref, at_b) in enumerate(spans):
            ahead = score(q, ref[at_b, 0:rows, 0:HEAD].reshape(k_blocks * rows, HEAD))
            state = absorb(state, ready, value)
            v_at = n_text + n * k_blocks * rows
            ready, value = ahead, v_scr[v_at : v_at + k_blocks * rows, :]
        top, acc = absorb(state, ready, value)
        finish(at, jnp.broadcast_to(top, (q_tile, HEAD)), acc[:, HEAD:], acc[:, 0:HEAD])
        return carry

    lax.fori_loop(0, q_ref.shape[0] // q_tile, tile, 0)


def attend_first_kernel(place_ref, own_ref, peer_ref, *refs, rows, texts, k_blocks):
    *q_refs, top_ref, total_ref, acc_ref, q_out, tk_scr, v_scr = refs
    here = lax.axis_index("seq") * lax.axis_size("tp") + lax.axis_index("tp")
    for r, ref in enumerate(q_refs):
        q_out[pl.ds(pl.multiple_of(place_ref[here, r] * rows, rows), rows), :] = ref[0:rows, 0:HEAD]

    def finish(at, top, total, acc):
        top_ref[at, :] = top
        total_ref[at, :] = total
        acc_ref[at, :] = acc

    attend(q_out, (own_ref, peer_ref), tk_scr, v_scr, rows, texts, 2 * rows, k_blocks, finish)


def attend_last_kernel(
    kv_ref, kv2_ref, top_ref, total_ref, acc_ref, q_ref, out_ref, tk_scr, v_scr, *, rows, texts, k_blocks
):
    def finish(at, top, total, acc):
        top_in, total_in = top_ref[at, :], total_ref[at, :]
        high = jnp.maximum(top, top_in)
        here, there = jnp.exp(top - high), jnp.exp(top_in - high)
        acc = acc * here + acc_ref[at, :] * there
        out_ref[at, :] = (acc / (total * here + total_in * there)).astype(jnp.bfloat16)

    attend(q_ref, (kv_ref, kv2_ref), tk_scr, v_scr, rows, texts, 2 * rows, k_blocks, finish)


def join_kernel(keep_ref, given_ref, *outs):
    rows = outs[0].shape[0] // 2
    for j, out in enumerate(outs):
        out[0:rows, :] = keep_ref[j * rows : (j + 1) * rows, :]
        out[rows:, :] = given_ref[j * rows : (j + 1) * rows, :]


def project_kernel(heads_ref, valid_ref, w_ref, *refs):
    *ins, mine_ref, other_ref, joined = refs
    share = mine_ref.shape[0]
    me = lax.axis_index("tp")
    here = lax.axis_index("seq") * lax.axis_size("tp") + me

    rows = joined.shape[0]
    for j, ref in enumerate(ins):

        @pl.when(valid_ref[here, j] == 1)
        def _():
            for h in range(2):
                at = pl.ds(pl.multiple_of(heads_ref[here, 2 * j + h] * HEAD, HEAD), HEAD)
                joined[:, at] = ref[h * rows : (h + 1) * rows, :]

    first = jnp.dot(joined[...], w_ref[...], preferred_element_type=jnp.float32).astype(jnp.bfloat16)
    low, high = first[:share], first[share:]
    mine_ref[...] = jnp.where(me == 0, low, high)
    other_ref[...] = jnp.where(me == 0, high, low)


def body(
    visual_q, visual_key_input, visual_v, text_k, text_v, text_mask, slab_order, q_gain, key_norm_gain, w_out
):
    rows, width = visual_q.shape
    texts = text_k.shape[0]
    heads = width // HEAD
    n_seq, n_tp = lax.axis_size("seq"), lax.axis_size("tp")
    perms, send, cross, flip, place, swap, perms_back, heads_back, valid = plan(n_seq, n_tp, heads)
    rounds, backs = len(perms), len(perms_back)
    both = ("seq", "tp")
    full = rows + texts
    vmem = pl.BlockSpec(memory_space=pltpu.VMEM)
    smem = pl.BlockSpec(memory_space=pltpu.SMEM)
    tables = position_tables(rows, n_seq * SLAB_H)
    half = rounds // 2
    got = []
    for first in (0, half):
        blocks = pl.pallas_call(
            functools.partial(prep_kernel, first=first),
            out_shape=[jax.ShapeDtypeStruct((full, 3 * HEAD), jnp.bfloat16)] * half,
            in_specs=[smem] * 3 + [vmem] * 11,
            out_specs=[vmem] * half,
            name="prep",
        )(
            send, text_mask, slab_order, visual_q, visual_key_input, visual_v, text_k, text_v, *tables,
            q_gain.reshape(1, HEAD), key_norm_gain.reshape(1, HEAD),
        )
        for r, b in enumerate(blocks, first):
            got.append(lax.ppermute(b, both, perms[r]))
    own = pl.pallas_call(
        pack_kernel,
        out_shape=jax.ShapeDtypeStruct((rounds, full + PAD, 2 * HEAD), jnp.bfloat16),
        in_specs=[vmem] * rounds,
        out_specs=vmem,
        name="pack",
    )(*got)
    across = lax.ppermute(own, both, cross)
    peer = lax.ppermute(own, both, flip)
    many = rounds * rows
    given = backs * rows
    text_scratch = [
        pltpu.VMEM((2 * rounds * (texts + PAD), HEAD), jnp.bfloat16),
        pltpu.VMEM((2 * rounds * (rows + texts + PAD), 2 * HEAD), jnp.bfloat16),
    ]
    *state, queries = pl.pallas_call(
        functools.partial(attend_first_kernel, rows=rows, texts=texts, k_blocks=rounds // 2),
        out_shape=[jax.ShapeDtypeStruct((many, HEAD), jnp.float32)] * 3
        + [jax.ShapeDtypeStruct((many, HEAD), jnp.bfloat16)],
        in_specs=[smem] + [vmem] * (2 + rounds),
        out_specs=[vmem] * 4,
        scratch_shapes=text_scratch,
        name="attention",
    )(place, own, peer, *got)
    peer_across = lax.ppermute(across, both, flip)

    def finish(part):
        block = pl.BlockSpec((given, HEAD), lambda i: (part, 0))
        whole_kv = pl.BlockSpec(own.shape, lambda i: (0, 0, 0))
        return pl.pallas_call(
            functools.partial(attend_last_kernel, rows=rows, texts=texts, k_blocks=rounds // 2),
            out_shape=jax.ShapeDtypeStruct((given, HEAD), jnp.bfloat16),
            grid=(1,),
            in_specs=[whole_kv] * 2 + [block] * 4,
            out_specs=pl.BlockSpec((given, HEAD), lambda i: (0, 0)),
            scratch_shapes=text_scratch,
            name="attention",
        )(across, peer_across, *state, queries)

    give = finish(0)
    taken = lax.ppermute(give, both, swap)
    keep = finish(1)
    outs = pl.pallas_call(
        join_kernel,
        out_shape=[jax.ShapeDtypeStruct((2 * rows, HEAD), jnp.bfloat16)] * backs,
        in_specs=[vmem] * 2,
        out_specs=[vmem] * backs,
        name="join",
    )(keep, taken)
    back = []
    for o, p in zip(outs, perms_back):
        back.append(lax.ppermute(o, both, p))
    share = rows // n_tp
    mine, other = pl.pallas_call(
        project_kernel,
        out_shape=[jax.ShapeDtypeStruct((share, w_out.shape[1]), jnp.bfloat16)] * 2,
        in_specs=[smem] * 2 + [vmem] * (1 + backs),
        out_specs=[vmem] * 2,
        scratch_shapes=[pltpu.VMEM((rows, width), jnp.bfloat16)],
        name="project",
    )(heads_back, valid, w_out, *back)
    theirs = lax.ppermute(other, "tp", [(0, 1), (1, 0)])
    return (mine.astype(jnp.float32) + theirs.astype(jnp.float32)).astype(jnp.bfloat16)


def solution(mesh):
    wide = P(("grp", "seq"), "tp")
    long = P(("grp", "seq"))
    placed = (wide, wide, wide, wide, wide, long, long, P(), P(), P("tp", None))
    return jax.shard_map(body, mesh=mesh, in_specs=placed, out_specs=P(("grp", "seq", "tp"), None), check_vma=False)
```
